32 devices in a mesh: gx: 4 (over y, core), gy: 2 (over x), gz: 4 (over z).
Axes of the slice: x: 2, y: 2, z: 4, core: 2. Of those that a mesh axis runs over, the one named last changes fastest.
Arguments:
- tokens: bfloat16 [32, 6144], P('gy'), may hold values from -6 to 6
- route: int32 [32, 2], P('gy'), may hold values from 0 to 3, all different within a row; in each aligned block of 16 rows (0 to 15, 16 to 31, ...) at most 12 rows name the same one
- weight_q: int32 [32, 2], P('gy'), may hold values from 1 to 65535
- w_gate: bfloat16 [4, 6144, 16384], P('gx', 'gy', 'gz'), may hold values from -0.078125 to 0.078125
- w_up: bfloat16 [4, 6144, 16384], P('gx', 'gy', 'gz'), may hold values from -0.078125 to 0.078125
- w_down: bfloat16 [4, 16384, 6144], P('gx', 'gz', 'gy'), may hold values from -0.046875 to 0.046875
Outputs:
- mixed: bfloat16 [32, 6144], P('gy', ('gx', 'gz'))
The draws below stay inside these ranges and needn't reach their ends.
Inputs may be any that keep to these rules, and one draw needn't show every extreme that they name: `route`: the 2 entries of a row are different; in each block of 16 rows owned by one index of gy no expert is named by more than 12 rows, a bound that some block reaches.
All inputs are finite; a program needn't handle non-finite values.
Results may differ from the reference program's by a relative error of at most 0.0049.
Values may be sent and summed in bfloat16 or wider, within the bound.
A program may use at most 256 MiB of HBM per device.

```python
import math
import jax
import jax.numpy as jnp
import numpy as np
from jax import lax

D = 6144
FF = 16384
TOK_OWN = 16
TOP = 2
CAP = 12
EXPERTS = 4
TOKENS = 32


def place_ends(drawn, own_key, smallest, largest):
    longest = drawn.shape.index(max(drawn.shape))
    spots = []
    for shift in (0, 1):
        where = [jax.random.randint(jax.random.fold_in(own_key, axis), (), 0, length) for axis, length in enumerate(drawn.shape)]
        where[longest] = (where[longest] + shift) % drawn.shape[longest]
        spots.append(tuple(where))
    return drawn.at[spots[0]].set(smallest).at[spots[1]].set(largest)


def shard_levels(key, shape, cuts, smallest, high):
    gain = 1.0
    for dim, parts in cuts:
        heights = jax.random.uniform(jax.random.fold_in(jax.random.fold_in(key, 6), dim), (parts,), jnp.float32, smallest / len(cuts), high / len(cuts))
        gain = gain * jnp.repeat(jnp.exp(heights), shape[dim] // parts).reshape((-1,) + (1,) * (len(shape) - 1 - dim))
    return gain


def assign_block(key, own, number, rows, count, top, most, slope):
    ranking = jax.random.permutation(key, count)
    heavy_load, usual = load_shares(count, rows * top, most, slope, True), load_shares(count, rows * top, most, slope, False)
    places = jnp.arange(count)

    def named(sizes, offset_by):
        used = int((sizes > 0).sum())
        fixed = max(1, used // 4)
        moved = fixed + (places - fixed + offset_by * (used - fixed)) % max(1, count - fixed)
        return jnp.zeros((count,), jnp.int32).at[ranking[jnp.where(places < fixed, places, moved)]].set(jnp.asarray(sizes, jnp.int32))

    sizes = jnp.where(number % 4 == 0, named(heavy_load, number // 4), named(usual, number - number // 4 - 1))
    mixed = jax.random.permutation(jax.random.fold_in(own, 3), count)
    donor, sink = mixed[0:count // 2 * 2:2], mixed[1:count // 2 * 2:2]
    slack = jnp.minimum(sizes[donor] - 1, most - sizes[sink]) // 2
    slack = jnp.where((donor == ranking[0]) | (sink == ranking[0]) | (sizes[sink] == 0), 0, jnp.maximum(slack, 0))
    moved = jax.random.randint(jax.random.fold_in(own, 4), (count // 2,), 0, 1 << 20) % (slack + 1)
    sizes = sizes.at[donor].add(-moved).at[sink].add(moved)
    labels = jnp.searchsorted(jnp.cumsum(sizes), jnp.arange(rows * top), side="right").astype(jnp.int32)
    table = labels.reshape(top, rows).T
    table = table[jax.random.permutation(jax.random.fold_in(own, 1), rows)]
    offset_by = jax.random.randint(jax.random.fold_in(own, 2), (rows, 1), 0, top)
    return jnp.take_along_axis(table, (jnp.arange(top)[None, :] + offset_by) % top, axis=1)


def load_shares(count, total, bound, lean, full):
    portions = [(1 << 20) // math.isqrt(standing ** lean) + 1 for standing in range(1, count + 1)]
    largest = bound if full else min(bound, max(-(-total // count), total * portions[0] // sum(portions)))
    least = 1 if total - largest >= count - 1 else 0
    given, surplus = [largest] + [least] * (count - 1), total - largest - least * (count - 1)
    while surplus > 0:
        free = [i for i in range(1, count) if given[i] < largest] or [i for i in range(1, count) if given[i] < bound]
        pool, budget = sum([portions[i] for i in free]), surplus
        for i in free:
            extra = min(bound - given[i], max(1, budget * portions[i] // pool), surplus)
            given[i] = given[i] + extra
            surplus = surplus - extra
    return np.array(given)


def scatter_about(key, shape, scale, most, shards=(), kind=jnp.bfloat16):
    array = jax.random.normal(key, shape, jnp.float32) * scale
    if len(shards) > 0:
        array = shard_levels(key, shape, shards, -0.22, 0.18) * array
    return jnp.clip(array, min=-most, max=most).astype(kind)


def setup_inputs(seed: int = 0) -> dict:
    splits = jax.random.split(jax.random.key(seed), 7)
    tokens = scatter_about(splits[0], (TOKENS, D), 1.0, 6.0, ((0, 2),))
    route_keys = jax.random.split(jax.random.fold_in(splits[1], 1), TOKENS // TOK_OWN)
    route_turns = jax.random.permutation(jax.random.fold_in(splits[1], 3), TOKENS // TOK_OWN)
    route = jax.vmap(lambda own, number: assign_block(jax.random.fold_in(splits[1], 2), own, number, TOK_OWN, EXPERTS, TOP, CAP, 2))(route_keys, route_turns).reshape((TOKENS, TOP))
    weight_q = place_ends(jax.random.randint(splits[2], (TOKENS, TOP), 1, 65536), jax.random.fold_in(splits[2], 1), 1, 65535).astype(jnp.int32)
    w_gate = scatter_about(splits[3], (EXPERTS, D, FF), D ** -0.5, 0.078125, ((0, 4), (1, 2), (2, 4)))
    w_up = scatter_about(splits[4], (EXPERTS, D, FF), D ** -0.5, 0.078125, ((0, 4), (1, 2), (2, 4)))
    w_down = scatter_about(splits[5], (EXPERTS, FF, D), FF ** -0.5, 0.046875, ((0, 4), (1, 4), (2, 2)))
    return {"tokens": tokens, "route": route, "weight_q": weight_q, "w_gate": w_gate, "w_up": w_up, "w_down": w_down}


def slot_table(owner_ids, expert):
    hits = (owner_ids == expert).astype(jnp.int32)
    routed = jnp.sum(hits, axis=-1)
    slot_index = jnp.cumsum(routed, axis=1) - 1
    columns = jnp.arange(CAP, dtype=jnp.int32)
    placing = (slot_index[:, None, :] == columns[None, :, None]) & (routed[:, None, :] > 0)
    return hits, placing


def reference(tokens, route, weight_q, w_gate, w_up, w_down):
    groups = TOKENS // TOK_OWN
    owner_ids = route.reshape(groups, TOK_OWN, TOP)
    owned = tokens.reshape(groups, TOK_OWN, D)
    weights_f = weight_q.astype(jnp.float32).reshape(groups, TOK_OWN, TOP)
    shares = weights_f / jnp.sum(weights_f, axis=-1, keepdims=True)
    positions = jnp.arange(TOK_OWN, dtype=jnp.int32)

    def one_expert(total, expert):
        hits, placing = slot_table(owner_ids, expert)
        place_full = placing.astype(jnp.float32)
        picked = jnp.sum(placing.astype(jnp.int32) * positions[None, None, :], axis=-1).astype(jnp.int32)
        filled = jnp.any(placing, axis=-1)
        rows = jnp.take_along_axis(owned, picked[:, :, None], axis=1)
        rows = rows * filled[:, :, None].astype(jnp.bfloat16)
        flat = rows.reshape(groups * CAP, D)
        gate = jnp.dot(flat, w_gate[expert], preferred_element_type=jnp.float32)
        upper = jnp.dot(flat, w_up[expert], preferred_element_type=jnp.float32)
        hidden = (jax.nn.silu(gate) * upper).astype(jnp.bfloat16)
        result = jnp.dot(hidden, w_down[expert], preferred_element_type=jnp.float32)
        token_gate = jnp.sum(hits.astype(jnp.float32) * shares, axis=-1)
        slot_gate = jnp.einsum("gct,gt->gc", place_full, token_gate, precision=lax.Precision.HIGHEST)
        weighted = slot_gate[:, :, None] * result.reshape(groups, CAP, D)
        back = jnp.einsum("gct,gcd->gtd", place_full, weighted, precision=lax.Precision.HIGHEST)
        return total + back, None

    start = jnp.zeros((groups, TOK_OWN, D), jnp.float32)
    total, _ = lax.scan(one_expert, start, jnp.arange(EXPERTS, dtype=jnp.int32))
    return total.reshape(TOKENS, D).astype(jnp.bfloat16)
```

```python
import jax
import jax.numpy as jnp
from jax import lax
from jax.sharding import PartitionSpec as P

CAP = 12


def per_device(tokens, route, weight_q, w_gate, w_up, w_down):
    expert = lax.axis_index("gx")
    width_z = lax.axis_size("gz")
    owners = lax.axis_size("gy")
    hits = (route == expert).astype(jnp.int32)
    routed = jnp.sum(hits, axis=1)
    slot_index = jnp.cumsum(routed) - 1
    columns = jnp.arange(CAP, dtype=jnp.int32)
    placing = (slot_index[None, :] == columns[:, None]) & (routed[None, :] > 0)
    place_half = placing.astype(jnp.bfloat16)
    place_full = placing.astype(jnp.float32)
    outgoing = jnp.dot(place_half, tokens, preferred_element_type=jnp.float32).astype(jnp.bfloat16)
    weights_f = weight_q.astype(jnp.float32)
    shares = weights_f / jnp.sum(weights_f, axis=1, keepdims=True)
    token_gate = jnp.sum(hits.astype(jnp.float32) * shares, axis=1)
    slot_gate = jnp.dot(place_full, token_gate, precision=lax.Precision.HIGHEST)
    depth = w_gate.shape[1]
    half = outgoing.reshape(CAP, owners, depth).transpose(1, 0, 2)
    piece = lax.all_to_all(half, "gy", split_axis=0, concat_axis=0, tiled=True)
    piece = piece.reshape(owners * CAP, depth)
    gate = jnp.dot(piece, w_gate[0], preferred_element_type=jnp.float32)
    upper = jnp.dot(piece, w_up[0], preferred_element_type=jnp.float32)
    both = lax.psum_scatter(jnp.stack([gate, upper]), "gy", scatter_dimension=2, tiled=True)
    hidden = (jax.nn.silu(both[0]) * both[1]).astype(jnp.bfloat16)
    down_local = w_down[0]
    partial_value = jnp.dot(
        lax.all_gather(hidden, "gy", axis=1, tiled=True),
        down_local,
        preferred_element_type=jnp.float32,
    )
    portion = CAP // width_z
    column_width = partial_value.shape[1]
    blocks = partial_value.reshape(owners, width_z, portion, column_width)
    narrowed = lax.psum_scatter(blocks, "gz", scatter_dimension=1, tiled=True)
    arrived = lax.all_to_all(narrowed, "gy", split_axis=0, concat_axis=1, tiled=True)
    full = jnp.transpose(arrived[0], (1, 0, 2)).reshape(portion, owners * column_width)
    first = lax.axis_index("gz") * portion
    gate_part = lax.dynamic_slice_in_dim(slot_gate, first, portion, 0)
    place_part = lax.dynamic_slice_in_dim(place_full, first, portion, 0)
    weighted = gate_part[:, None] * full
    contribution = jnp.dot(place_part.T, weighted, precision=lax.Precision.HIGHEST)
    result = lax.psum_scatter(contribution, ("gx", "gz"), scatter_dimension=1, tiled=True)
    return result.astype(jnp.bfloat16)


def solution(mesh):
    in_specs = (
        P("gy", None),
        P("gy", None),
        P("gy", None),
        P("gx", "gy", "gz"),
        P("gx", "gy", "gz"),
        P("gx", "gz", "gy"),
    )
    out_specs = P("gy", ("gx", "gz"))
    return jax.shard_map(
        per_device, mesh=mesh, in_specs=in_specs, out_specs=out_specs, check_vma=False
    )
```
